32 devices in a mesh: row: 4 (over y, core), col: 8 (over z, x).
Axes of the slice: x: 2, y: 2, z: 4, core: 2. Of those that a mesh axis runs over, the one named last changes fastest.
Arguments:
- nodes: bfloat16 [32768, 512], P(('row', 'col')), may hold values from -8 to 8
- ln1_gain: float32 [512], replicated, may hold values from 0.25 to 1.75
- w_qkv: bfloat16 [512, 1536], replicated, may hold values from -1 to 1
- w_out: bfloat16 [512, 512], replicated, may hold values from -0.25 to 0.25
- ln2_gain: float32 [512], replicated, may hold values from 0.25 to 1.75
- w_up: bfloat16 [512, 2048], replicated, may hold values from -0.25 to 0.25
- w_down: bfloat16 [2048, 512], replicated, may hold values from -0.125 to 0.125
- adjacency: int32 [32768, 128], P(('row', 'col')), may hold values 0 or 1
- remote_ids: int32 [32, 10], replicated, may hold values from 0 to 255, as said below
- remote_live: int32 [32, 10], replicated, may hold values from 0 to 1, as said below
Outputs:
- updated: bfloat16 [32768, 512], P(('row', 'col'))
The draws below stay inside these ranges and needn't reach their ends.
Inputs may be any that keep to these rules, and one draw needn't show every extreme that they name: `remote_ids`: every entry of device d's list names a block of another device in d's row or d's column of the mesh; the entries of one list are distinct; at most 1 live entries of one list name blocks of one device, and some list has exactly 1 from one device. `remote_live`: some device has all 10 entries live; every device has 8 or more.
All inputs are finite; a program needn't handle non-finite values. No bound on the sum of `adjacency` on one device may be relied on, other than what follows from the above.
Results may differ from the reference program's by a relative error of at most 0.005.
Values may be sent and summed in bfloat16 or wider, within the bound.
A program may use at most 128 MiB of HBM per device.

```python
import math
import jax
import jax.numpy as jnp
from jax import lax

D = 512
HEADS = 8
FF = 2048
BLK = 128
NODE_DEV = 1024
SLOTS = 10
CAP = 1
NODES = 32768
N_ROW = 4
N_COL = 8


def plan_lists(key):
    local_blocks = NODE_DEV // BLK
    peer_total = N_ROW + N_COL - 2
    picks_count = SLOTS // CAP

    def one_device(device):
        subkey = jax.random.fold_in(key, device)
        my_row = device // N_COL
        my_col = device % N_COL
        peer_order = jnp.arange(peer_total, dtype=jnp.int32)
        in_row = peer_order < N_COL - 1
        col_pick = peer_order + (peer_order >= my_col).astype(jnp.int32)
        row_base = peer_order - (N_COL - 1)
        row_pick = row_base + (row_base >= my_row).astype(jnp.int32)
        peers = jnp.where(in_row, my_row * N_COL + col_pick, row_pick * N_COL + my_col)
        chosen = jax.random.permutation(jax.random.fold_in(subkey, 1), peers)[:picks_count]
        block_keys = jax.random.split(jax.random.fold_in(subkey, 2), picks_count)
        picked = jax.vmap(lambda one_key: jax.random.permutation(one_key, local_blocks)[:CAP])(block_keys)
        block_ids = (chosen[:, None] * local_blocks + picked.astype(jnp.int32)).reshape(-1)
        block_ids = jax.random.permutation(jax.random.fold_in(subkey, 3), block_ids)
        live_count = jax.random.randint(jax.random.fold_in(subkey, 4), (), SLOTS - 2, SLOTS + 1)
        live_count = jnp.where(device == 0, SLOTS, live_count)
        alive_row = (jnp.arange(SLOTS, dtype=jnp.int32) < live_count).astype(jnp.int32)
        return (block_ids.astype(jnp.int32), alive_row)
    return jax.vmap(one_device)(jnp.arange(N_ROW * N_COL, dtype=jnp.int32))


def draw_remote_ids(key, part):
    return plan_lists(jax.random.fold_in(key, 77))[0]


def draw_remote_live(key, part):
    return plan_lists(jax.random.fold_in(key, 77))[1]


def draw_nodes(key, part):
    noise = jax.random.normal(jax.random.fold_in(key, 501), (NODES, D), jnp.float32)
    values = jnp.clip(noise, -6.0, 6.0)
    return values.astype(jnp.bfloat16)


def draw_w_qkv(key, part):
    values = jnp.clip(jax.random.normal(jax.random.fold_in(key, 601), (D, 3 * D), jnp.float32), -6.0, 6.0) * (1.0 / math.sqrt(D))
    return values.astype(jnp.bfloat16)


def with_ends(drawn, rng, low, largest):
    spot = [jax.random.randint(jax.random.fold_in(rng, axis), (), 0, length) for axis, length in enumerate(drawn.shape)]
    main_axis = drawn.shape.index(max(drawn.shape))
    neighbour = spot[:main_axis] + [(spot[main_axis] + 1) % drawn.shape[main_axis]] + spot[main_axis + 1:]
    return drawn.at[tuple(spot)].set(low).at[tuple(neighbour)].set(largest)


def bell_draw(own_key, dims, deviation, most, kind=jnp.bfloat16):
    array = jax.random.normal(own_key, dims, jnp.float32) * deviation
    return jnp.minimum(jnp.maximum(array, -most), most).astype(kind)


def setup_inputs(seed: int = 0) -> dict:
    keys = jax.random.split(jax.random.key(seed), 11)
    nodes = draw_nodes(jax.random.fold_in(keys[10], 71), 0)
    ln1_gain = jnp.clip(1.0 + 0.15 * jax.random.normal(keys[1], (D,), jnp.float32), 0.25, 1.75)
    w_qkv = draw_w_qkv(jax.random.fold_in(keys[10], 71), 0)
    w_out = bell_draw(keys[3], (D, D), D ** -0.5, 0.25)
    ln2_gain = jnp.clip(1.0 + 0.15 * jax.random.normal(keys[4], (D,), jnp.float32), 0.25, 1.75)
    w_up = bell_draw(keys[5], (D, FF), D ** -0.5, 0.25)
    w_down = bell_draw(keys[6], (FF, D), FF ** -0.5, 0.125)
    adjacency = with_ends((jax.random.randint(keys[7], (NODES, BLK), 0, 4) < 1).astype(jnp.int32), jax.random.fold_in(keys[7], 1), 0, 1)
    remote_ids = draw_remote_ids(jax.random.fold_in(keys[10], 71), 0)
    remote_live = draw_remote_live(jax.random.fold_in(keys[10], 71), 0)
    return dict(nodes=nodes, ln1_gain=ln1_gain, w_qkv=w_qkv, w_out=w_out, ln2_gain=ln2_gain, w_up=w_up, w_down=w_down, adjacency=adjacency, remote_ids=remote_ids, remote_live=remote_live)


EPS = 1e-05
NEG_FILL = -1e+30

def normalize(values, gain):
    values = values.astype(jnp.float32)
    row_mean = lax.optimization_barrier(jnp.mean(values, axis=-1, keepdims=True))
    centered = values - row_mean
    row_var = lax.optimization_barrier(jnp.mean(centered * centered, axis=-1, keepdims=True))
    return (centered * lax.rsqrt(row_var + EPS) * gain).astype(jnp.bfloat16)

def attend(queries, local_kv, remote_kv, adj_rows, key_alive):
    row_count = queries.shape[0]
    model_width = queries.shape[1]
    head_dim = model_width // HEADS
    block_count = row_count // BLK
    score_scale = 1.0 / math.sqrt(head_dim)
    query_f = queries.astype(jnp.float32).reshape(block_count, BLK, HEADS, head_dim)
    local_keys = local_kv[:, :model_width].astype(jnp.float32).reshape(block_count, BLK, HEADS, head_dim)
    local_vals = local_kv[:, model_width:].astype(jnp.float32).reshape(block_count, BLK, HEADS, head_dim)
    remote_keys = remote_kv[:, :model_width].astype(jnp.float32).reshape(-1, HEADS, head_dim)
    remote_vals = remote_kv[:, model_width:].astype(jnp.float32).reshape(-1, HEADS, head_dim)
    local_scores = jnp.einsum('bihd,bjhd->bhij', query_f, local_keys) * score_scale
    eye_mask = jnp.arange(BLK)[:, None] == jnp.arange(BLK)[None, :]
    allowed = (adj_rows.reshape(block_count, BLK, BLK) > 0) | eye_mask[None]
    local_scores = jnp.where(allowed[:, None], local_scores, NEG_FILL)
    remote_scores = jnp.einsum('bihd,jhd->bhij', query_f, remote_keys) * score_scale
    remote_scores = jnp.where(key_alive[None, None, None, :] > 0, remote_scores, NEG_FILL)
    row_max = jnp.maximum(lax.optimization_barrier(jnp.max(local_scores, axis=-1)), lax.optimization_barrier(jnp.max(remote_scores, axis=-1)))
    local_exp = jnp.exp(local_scores - row_max[..., None])
    remote_exp = jnp.exp(remote_scores - row_max[..., None])
    row_total = lax.optimization_barrier(jnp.sum(local_exp, axis=-1)) + lax.optimization_barrier(jnp.sum(remote_exp, axis=-1))
    local_probs = (local_exp / row_total[..., None]).astype(jnp.bfloat16).astype(jnp.float32)
    remote_probs = (remote_exp / row_total[..., None]).astype(jnp.bfloat16).astype(jnp.float32)
    summed = jnp.einsum('bhij,bjhd->bihd', local_probs, local_vals) + jnp.einsum('bhij,jhd->bihd', remote_probs, remote_vals)
    return summed.reshape(row_count, model_width).astype(jnp.bfloat16)

def reference(nodes, ln1_gain, w_qkv, w_out, ln2_gain, w_up, w_down, adjacency, remote_ids, remote_live):
    model_width = nodes.shape[1]
    device_count = remote_ids.shape[0]
    node_count = nodes.shape[0] // device_count
    normed = normalize(nodes, ln1_gain)
    projected = jnp.dot(normed, w_qkv, preferred_element_type=jnp.float32).astype(jnp.bfloat16)
    keyval = projected[:, model_width:]
    all_blocks = keyval.reshape(-1, BLK, 2 * model_width)

    def one_device(device):
        start = (device * node_count).astype(jnp.int32)
        queries = lax.dynamic_slice_in_dim(projected, start, node_count, 0)[:, :model_width]
        local_kv = lax.dynamic_slice_in_dim(keyval, start, node_count, 0)
        adj_rows = lax.dynamic_slice_in_dim(adjacency, start, node_count, 0)
        block_ids = lax.dynamic_index_in_dim(remote_ids, device, 0, keepdims=False)
        alive_row = lax.dynamic_index_in_dim(remote_live, device, 0, keepdims=False)
        remote_kv = jnp.take(all_blocks, block_ids, axis=0).reshape(-1, 2 * model_width)
        key_alive = jnp.repeat(alive_row, BLK)
        return attend(queries, local_kv, remote_kv, adj_rows, key_alive)
    mixed = lax.map(one_device, jnp.arange(device_count, dtype=jnp.int32)).reshape(-1, model_width)
    residual = nodes.astype(jnp.float32) + jnp.dot(mixed, w_out, preferred_element_type=jnp.float32)
    normed_two = normalize(residual, ln2_gain)
    upward = jnp.dot(normed_two, w_up, preferred_element_type=jnp.float32)
    activated = jax.nn.gelu(upward, approximate=True).astype(jnp.bfloat16)
    return (residual + jnp.dot(activated, w_down, preferred_element_type=jnp.float32)).astype(jnp.bfloat16)
```

```python
import functools
import math

import jax
import jax.numpy as jnp
from jax import lax
from jax.experimental import pallas as pl
from jax.experimental.pallas import tpu as pltpu
from jax.sharding import PartitionSpec as P

HEADS = 8
BLK = 128
HEAD_DIM = 64
AUG = 80
EPS = 1e-05
NEG_FILL = -1e30
LOG2E = 1.4426950408889634
MESH = pl.DeviceIdType.MESH
NT = (((1,), (1,)), ((), ()))


def dot(a, b):
    return jnp.dot(a, b, preferred_element_type=jnp.float32)


def dot_nt(a, b):
    return lax.dot_general(a, b, NT, preferred_element_type=jnp.float32)


def normalize(values, gain):
    values = values.astype(jnp.float32)
    row_mean = jnp.mean(values, axis=-1, keepdims=True)
    centered = values - row_mean
    row_var = jnp.mean(centered * centered, axis=-1, keepdims=True)
    return (centered * lax.rsqrt(row_var + EPS) * gain).astype(jnp.bfloat16)


def peer_offsets(row_size, col_size):
    return [("row", d) for d in range(1, row_size)] + [("col", d) for d in range(1, col_size)]


def attention_kernel(
    row_size, col_size,
    ids_ref, live_ref, nodes_ref, gain_ref, w_ref, adj_ref,
    mixed_ref,
    send_buf, recv_buf, dead_ref, wq_t, wv_t, q_t, keys, vals_t, keys_r, vals_r, bias_t, top, acc,
    send_sem, recv_sem,
):
    rows, width = nodes_ref.shape
    local_blocks = rows // BLK
    slots = ids_ref.shape[1]
    pairs = HEADS // 2
    my_row = lax.axis_index("row")
    my_col = lax.axis_index("col")
    me = my_row * col_size + my_col
    offsets = peer_offsets(row_size, col_size)
    count = len(offsets)
    group = 2 if count % 2 == 0 else 1

    def target(axis, d):
        if axis == "row":
            return lax.rem(my_row + d, row_size), my_col
        return my_row, lax.rem(my_col + d, col_size)

    def source(axis, d):
        if axis == "row":
            return lax.rem(my_row + row_size - d, row_size), my_col
        return my_row, lax.rem(my_col + col_size - d, col_size)

    barrier = pltpu.get_barrier_semaphore()
    for axis, d in offsets:
        pl.semaphore_signal(barrier, inc=1, device_id=target(axis, d), device_id_type=MESH)
    for p, (axis, d) in enumerate(offsets):
        t_row, t_col = target(axis, d)
        peer = t_row * col_size + t_col
        base = me * local_blocks
        picked = jnp.zeros((BLK, width), jnp.bfloat16)
        for b in range(local_blocks):
            hits = jnp.int32(0)
            for s in range(slots):
                hit = (live_ref[peer, s] > 0) & (ids_ref[peer, s] == base + b)
                hits = jnp.maximum(hits, hit.astype(jnp.int32))
            weight = jnp.full((1, width), hits).astype(jnp.bfloat16)
            picked = picked + nodes_ref[b * BLK : (b + 1) * BLK, :] * weight
        send_buf[p] = picked
    pl.semaphore_wait(barrier, count)

    def copy(p, device):
        return pltpu.make_async_remote_copy(
            src_ref=send_buf.at[p], dst_ref=recv_buf.at[p],
            send_sem=send_sem.at[p], recv_sem=recv_sem.at[p],
            device_id=device, device_id_type=MESH,
        )

    for p, (axis, d) in enumerate(offsets):
        copy(p, target(axis, d)).start()

    for p, (axis, d) in enumerate(offsets):
        s_row, s_col = source(axis, d)
        first = (s_row * col_size + s_col) * local_blocks
        dead = jnp.float32(NEG_FILL)
        for s in range(slots):
            block = ids_ref[me, s] - first
            hit = (live_ref[me, s] > 0) & (block >= 0) & (block < local_blocks)
            dead = jnp.where(hit, jnp.float32(0), dead)
        dead_ref[p] = dead

    gain = gain_ref[...]
    wq_t[...] = w_ref[:, :width].T
    wv_t[...] = w_ref[:, 2 * width :].T
    chunk = 2 * BLK
    score_scale = LOG2E / math.sqrt(HEAD_DIM)
    zeros = jnp.zeros((HEAD_DIM, chunk), jnp.bfloat16)
    vals_t[:, HEAD_DIM:, :] = jnp.ones((HEADS, AUG - HEAD_DIM, rows), jnp.bfloat16)
    vals_r[:, HEAD_DIM:, :] = jnp.ones((HEADS, AUG - HEAD_DIM, group * BLK), jnp.bfloat16)

    def project_local(i, carry):
        span = pl.ds(pl.multiple_of(i * chunk, chunk), chunk)
        normed = normalize(nodes_ref[span, :], gain)
        query = (dot_nt(wq_t[...], normed) * score_scale).astype(jnp.bfloat16)
        for h in range(HEADS):
            own = (h % 2) * HEAD_DIM
            q_t[h, own : own + HEAD_DIM, span] = query[h * HEAD_DIM : (h + 1) * HEAD_DIM]
            q_t[h, HEAD_DIM - own : 2 * HEAD_DIM - own, span] = zeros
        key = dot(normed, w_ref[:, width : 2 * width]).astype(jnp.bfloat16)
        for j in range(pairs):
            keys[j, span, :] = key[:, j * BLK : (j + 1) * BLK]
        value = dot_nt(wv_t[...], normed).astype(jnp.bfloat16)
        for h in range(HEADS):
            vals_t[h, :HEAD_DIM, span] = value[h * HEAD_DIM : (h + 1) * HEAD_DIM]
        return carry

    lax.fori_loop(0, rows // chunk, project_local, 0)

    eye = lax.broadcasted_iota(jnp.int32, (BLK, BLK), 0) == lax.broadcasted_iota(
        jnp.int32, (BLK, BLK), 1
    )
    for b in range(local_blocks):
        allowed = (adj_ref[b * BLK : (b + 1) * BLK, :] > 0) | eye
        bias_t[:, b * BLK : (b + 1) * BLK] = jnp.where(allowed, 0.0, NEG_FILL).T

    def attend_local(h, carry):
        for b in range(local_blocks):
            span = slice(b * BLK, (b + 1) * BLK)
            score = dot(keys[h // 2, span, :], q_t[h, :, span]) + bias_t[:, span]
            high = jnp.max(score, axis=0, keepdims=True)
            prob = jnp.exp2(score - high).astype(jnp.bfloat16)
            top[h, :, span] = high
            acc[h, :, span] = dot(vals_t[h, :, span], prob)
        return carry

    lax.fori_loop(0, HEADS, attend_local, 0)

    def attend_remote(g, carry):
        for k in range(group):
            copy(g * group + k, (my_row, my_col)).wait_recv()
        for k in range(group):
            span = slice(k * BLK, (k + 1) * BLK)
            normed = normalize(recv_buf[g * group + k], gain)
            key = dot(normed, w_ref[:, width : 2 * width]).astype(jnp.bfloat16)
            for j in range(pairs):
                keys_r[j, span, :] = key[:, j * BLK : (j + 1) * BLK]
            value = dot_nt(wv_t[...], normed).astype(jnp.bfloat16)
            for h in range(HEADS):
                vals_r[h, :HEAD_DIM, span] = value[h * HEAD_DIM : (h + 1) * HEAD_DIM]
        deads = [dead_ref[g * group + k] for k in range(group)]

        def one_head(h, inner):
            for c in range(rows // chunk):
                span = slice(c * chunk, (c + 1) * chunk)
                score = dot(keys_r[h // 2], q_t[h, :, span])
                parts = [score[k * BLK : (k + 1) * BLK] for k in range(group)]
                old = top[h, :, span]
                high = old
                for part, dead in zip(parts, deads):
                    high = jnp.maximum(high, jnp.max(part, axis=0, keepdims=True) + dead)
                prob = jnp.concatenate(
                    [
                        jnp.exp2(part - (high - dead)).astype(jnp.bfloat16)
                        for part, dead in zip(parts, deads)
                    ],
                    axis=0,
                )
                top[h, :, span] = high
                acc[h, :, span] = acc[h, :, span] * jnp.exp2(old - high) + dot(vals_r[h], prob)
            return inner

        return lax.fori_loop(0, HEADS, one_head, carry)

    lax.fori_loop(0, count // group, attend_remote, 0)

    def finish(h, carry):
        total = acc[h, HEAD_DIM : HEAD_DIM + 1, :]
        mixed_ref[h] = (acc[h, :HEAD_DIM, :] / total).astype(jnp.bfloat16)
        return carry

    lax.fori_loop(0, HEADS, finish, 0)
    for p, (axis, d) in enumerate(offsets):
        copy(p, target(axis, d)).wait_send()


def feed_kernel(mixed_ref, nodes_ref, w_out_ref, gain_ref, w_up_ref, w_down_ref, out_ref):
    mixed_t = mixed_ref[...].reshape(nodes_ref.shape[1], nodes_ref.shape[0])
    residual = nodes_ref[...].astype(jnp.float32) + dot(mixed_t.T, w_out_ref[...])
    normed = normalize(residual, gain_ref[...])
    upward = dot(normed, w_up_ref[...])
    activated = jax.nn.gelu(upward, approximate=True).astype(jnp.bfloat16)
    out_ref[...] = (residual + dot(activated, w_down_ref[...])).astype(jnp.bfloat16)


def shards(
    row_size, col_size,
    nodes, ln1_gain, w_qkv, w_out, ln2_gain, w_up, w_down, adjacency, remote_ids, remote_live
):
    rows, width = nodes.shape
    count = row_size + col_size - 2
    group = 2 if count % 2 == 0 else 1
    vmem = pl.BlockSpec(memory_space=pltpu.VMEM)
    smem = pl.BlockSpec(memory_space=pltpu.SMEM)
    bf16, f32 = jnp.bfloat16, jnp.float32
    mixed = pl.pallas_call(
        functools.partial(attention_kernel, row_size, col_size),
        out_shape=jax.ShapeDtypeStruct((HEADS, HEAD_DIM, rows), bf16),
        in_specs=[smem, smem, vmem, vmem, vmem, vmem],
        out_specs=vmem,
        scratch_shapes=[
            pltpu.VMEM((count, BLK, width), bf16),
            pltpu.VMEM((count, BLK, width), bf16),
            pltpu.SMEM((count,), f32),
            pltpu.VMEM((width, width), bf16),
            pltpu.VMEM((width, width), bf16),
            pltpu.VMEM((HEADS, 2 * HEAD_DIM, rows), bf16),
            pltpu.VMEM((HEADS // 2, rows, BLK), bf16),
            pltpu.VMEM((HEADS, AUG, rows), bf16),
            pltpu.VMEM((HEADS // 2, group * BLK, BLK), bf16),
            pltpu.VMEM((HEADS, AUG, group * BLK), bf16),
            pltpu.VMEM((BLK, rows), f32),
            pltpu.VMEM((HEADS, 1, rows), f32),
            pltpu.VMEM((HEADS, AUG, rows), f32),
            pltpu.SemaphoreType.DMA((count,)),
            pltpu.SemaphoreType.DMA((count,)),
        ],
        compiler_params=pltpu.CompilerParams(
            collective_id=0, has_side_effects=True, vmem_limit_bytes=40 << 20
        ),
        name="attention",
    )(remote_ids, remote_live, nodes, ln1_gain.reshape(1, width), w_qkv, adjacency)
    chunk = 2 * BLK
    hidden = w_up.shape[1]
    whole = lambda *dims: pl.BlockSpec(dims, lambda i: (0,) * len(dims))
    return pl.pallas_call(
        feed_kernel,
        grid=(rows // chunk,),
        out_shape=jax.ShapeDtypeStruct((rows, width), bf16),
        in_specs=[
            pl.BlockSpec((HEADS, HEAD_DIM, chunk), lambda i: (0, 0, i)),
            pl.BlockSpec((chunk, width), lambda i: (i, 0)),
            whole(width, width),
            whole(1, width),
            whole(width, hidden),
            whole(hidden, width),
        ],
        out_specs=pl.BlockSpec((chunk, width), lambda i: (i, 0)),
        compiler_params=pltpu.CompilerParams(vmem_limit_bytes=40 << 20),
        name="feed",
    )(mixed, nodes, w_out, ln2_gain.reshape(1, width), w_up, w_down)


def solution(mesh):
    split = P(("row", "col"), None)
    return jax.shard_map(
        functools.partial(shards, mesh.shape["row"], mesh.shape["col"]),
        mesh=mesh,
        in_specs=(split, P(), P(), P(), P(), P(), P(), split, P(), P()),
        out_specs=split,
        check_vma=False,
    )
```

```python
import functools
import math

import jax
import jax.numpy as jnp
from jax import lax
from jax.experimental import pallas as pl
from jax.experimental.pallas import tpu as pltpu
from jax.sharding import PartitionSpec as P

HEADS = 8
BLK = 128
HEAD_DIM = 64
AUG = 80
EPS = 1e-05
NEG_FILL = -1e30
LOG2E = 1.4426950408889634
MESH = pl.DeviceIdType.MESH
NT = (((1,), (1,)), ((), ()))


def dot(a, b):
    return jnp.dot(a, b, preferred_element_type=jnp.float32)


def dot_nt(a, b):
    return lax.dot_general(a, b, NT, preferred_element_type=jnp.float32)


def normalize(values, gain):
    values = values.astype(jnp.float32)
    row_mean = jnp.mean(values, axis=-1, keepdims=True)
    centered = values - row_mean
    row_var = jnp.mean(centered * centered, axis=-1, keepdims=True)
    return (centered * lax.rsqrt(row_var + EPS) * gain).astype(jnp.bfloat16)


def peer_offsets(row_size, col_size):
    return [("row", d) for d in range(1, row_size)] + [("col", d) for d in range(1, col_size)]


def attention_kernel(
    row_size, col_size,
    ids_ref, live_ref, nodes_hbm, gain_ref, w_hbm, adj_hbm,
    mixed_ref,
    nodes_ref, w_ref, adj_ref,
    send_buf, recv_buf, dead_ref, wq_t, wv_t, q_t, keys, vals_t, keys_r, vals_r, bias_t, top, acc,
    send_sem, recv_sem, load_sem,
):
    loads = [
        pltpu.make_async_copy(hbm, ref, load_sem.at[i])
        for i, (hbm, ref) in enumerate(((nodes_hbm, nodes_ref), (w_hbm, w_ref), (adj_hbm, adj_ref)))
    ]
    for load in loads:
        load.start()
    rows, width = nodes_ref.shape
    local_blocks = rows // BLK
    slots = ids_ref.shape[1]
    pairs = HEADS // 2
    my_row = lax.axis_index("row")
    my_col = lax.axis_index("col")
    me = my_row * col_size + my_col
    offsets = peer_offsets(row_size, col_size)
    count = len(offsets)
    group = 2 if count % 2 == 0 else 1

    def partner(me_there, d, size, sign):
        if size & (size - 1) == 0:
            flipped = me_there
            bit = 1
            while bit < size:
                if d & bit:
                    flipped = flipped + bit - 2 * bit * lax.rem(me_there // bit, 2)
                bit *= 2
            return flipped
        return lax.rem(me_there + size + sign * d, size)

    def target(axis, d):
        if axis == "row":
            return partner(my_row, d, row_size, 1), my_col
        return my_row, partner(my_col, d, col_size, 1)

    def source(axis, d):
        if axis == "row":
            return partner(my_row, d, row_size, -1), my_col
        return my_row, partner(my_col, d, col_size, -1)

    barrier = pltpu.get_barrier_semaphore()
    for axis, d in offsets:
        pl.semaphore_signal(barrier, inc=1, device_id=target(axis, d), device_id_type=MESH)
    loads[0].wait()
    for p, (axis, d) in enumerate(offsets):
        t_row, t_col = target(axis, d)
        peer = t_row * col_size + t_col
        base = me * local_blocks
        picked = jnp.zeros((BLK, width), jnp.bfloat16)
        for b in range(local_blocks):
            hits = jnp.int32(0)
            for s in range(slots):
                hit = (live_ref[peer, s] > 0) & (ids_ref[peer, s] == base + b)
                hits = jnp.maximum(hits, hit.astype(jnp.int32))
            weight = jnp.full((1, width), hits).astype(jnp.bfloat16)
            picked = picked + nodes_ref[b * BLK : (b + 1) * BLK, :] * weight
        send_buf[p] = picked
    pl.semaphore_wait(barrier, count)

    def copy(p, device):
        return pltpu.make_async_remote_copy(
            src_ref=send_buf.at[p], dst_ref=recv_buf.at[p],
            send_sem=send_sem.at[p], recv_sem=recv_sem.at[p],
            device_id=device, device_id_type=MESH,
        )

    for p, (axis, d) in enumerate(offsets):
        copy(p, target(axis, d)).start()

    for p, (axis, d) in enumerate(offsets):
        s_row, s_col = source(axis, d)
        first = (s_row * col_size + s_col) * local_blocks
        dead = jnp.float32(NEG_FILL)
        for s in range(slots):
            block = ids_ref[me, s] - first
            hit = (live_ref[me, s] > 0) & (block >= 0) & (block < local_blocks)
            dead = jnp.where(hit, jnp.float32(0), dead)
        dead_ref[p] = dead

    loads[1].wait()
    loads[2].wait()
    gain = gain_ref[...]
    wq_t[...] = w_ref[:, :width].T
    wv_t[...] = w_ref[:, 2 * width :].T
    chunk = 2 * BLK
    wide = 2 * BLK
    score_scale = LOG2E / math.sqrt(HEAD_DIM)
    zeros = jnp.zeros((HEAD_DIM, chunk), jnp.bfloat16)
    vals_t[:, HEAD_DIM:, :] = jnp.ones((HEADS, AUG - HEAD_DIM, rows), jnp.bfloat16)
    vals_r[:, HEAD_DIM:, :] = jnp.ones((HEADS, AUG - HEAD_DIM, group * BLK), jnp.bfloat16)

    def project_local(i, carry):
        span = pl.ds(pl.multiple_of(i * chunk, chunk), chunk)
        normed = normalize(nodes_ref[span, :], gain)
        query = (dot_nt(wq_t[...], normed) * score_scale).astype(jnp.bfloat16)
        for h in range(HEADS):
            own = (h % 2) * HEAD_DIM
            q_t[h, own : own + HEAD_DIM, span] = query[h * HEAD_DIM : (h + 1) * HEAD_DIM]
            q_t[h, HEAD_DIM - own : 2 * HEAD_DIM - own, span] = zeros
        key = dot(normed, w_ref[:, width : 2 * width]).astype(jnp.bfloat16)
        for j in range(pairs):
            keys[j, span, :] = key[:, j * BLK : (j + 1) * BLK]
        value = dot_nt(wv_t[...], normed).astype(jnp.bfloat16)
        for h in range(HEADS):
            vals_t[h, :HEAD_DIM, span] = value[h * HEAD_DIM : (h + 1) * HEAD_DIM]
        return carry

    lax.fori_loop(0, rows // chunk, project_local, 0)

    eye = lax.broadcasted_iota(jnp.int32, (BLK, BLK), 0) == lax.broadcasted_iota(
        jnp.int32, (BLK, BLK), 1
    )
    for b in range(local_blocks):
        allowed = (adj_ref[b * BLK : (b + 1) * BLK, :] > 0) | eye
        bias_t[:, b * BLK : (b + 1) * BLK] = jnp.where(allowed, 0.0, NEG_FILL).T

    def attend_local(h, carry):
        spans = [slice(b * BLK, (b + 1) * BLK) for b in range(local_blocks)]
        scores = [dot(keys[h // 2, span, :], q_t[h, :, span]) + bias_t[:, span] for span in spans]
        highs = [jnp.max(score, axis=0, keepdims=True) for score in scores]
        probs = [jnp.exp2(score - high).astype(jnp.bfloat16) for score, high in zip(scores, highs)]
        news = [dot(vals_t[h, :, span], prob) for span, prob in zip(spans, probs)]
        for span, high, new in zip(spans, highs, news):
            top[h, :, span] = high
            acc[h, :, span] = new
        return carry

    lax.fori_loop(0, HEADS, attend_local, 0)

    def attend_remote(g, carry):
        for k in range(group):
            copy(g * group + k, (my_row, my_col)).wait_recv()
        for k in range(group):
            span = slice(k * BLK, (k + 1) * BLK)
            normed = normalize(recv_buf[g * group + k], gain)
            key = dot(normed, w_ref[:, width : 2 * width]).astype(jnp.bfloat16)
            for j in range(pairs):
                keys_r[j, span, :] = key[:, j * BLK : (j + 1) * BLK]
            value = dot_nt(wv_t[...], normed).astype(jnp.bfloat16)
            for h in range(HEADS):
                vals_r[h, :HEAD_DIM, span] = value[h * HEAD_DIM : (h + 1) * HEAD_DIM]
        deads = [dead_ref[g * group + k] for k in range(group)]

        def one_head(h, inner):
            spans = [slice(c * wide, (c + 1) * wide) for c in range(rows // wide)]
            olds = [top[h, :, span] for span in spans]
            sums = [acc[h, :, span] for span in spans]
            value = vals_r[h]
            scores = [dot(keys_r[h // 2], q_t[h, :, span]) for span in spans]
            highs = []
            for score, old in zip(scores, olds):
                high = old
                for k, dead in enumerate(deads):
                    part = score[k * BLK : (k + 1) * BLK]
                    high = jnp.maximum(high, jnp.max(part, axis=0, keepdims=True) + dead)
                highs.append(high)
            probs = [
                jnp.concatenate(
                    [
                        jnp.exp2(score[k * BLK : (k + 1) * BLK] - (high - dead)).astype(jnp.bfloat16)
                        for k, dead in enumerate(deads)
                    ],
                    axis=0,
                )
                for score, high in zip(scores, highs)
            ]
            news = [dot(value, prob) for prob in probs]
            for span, old, high, before, new in zip(spans, olds, highs, sums, news):
                top[h, :, span] = high
                acc[h, :, span] = before * jnp.exp2(old - high) + new
            return inner

        return lax.fori_loop(0, HEADS, one_head, carry)

    lax.fori_loop(0, count // group, attend_remote, 0)

    def finish(h, carry):
        total = acc[h, HEAD_DIM : HEAD_DIM + 1, :]
        mixed_ref[h] = (acc[h, :HEAD_DIM, :] / total).astype(jnp.bfloat16)
        return carry

    lax.fori_loop(0, HEADS, finish, 0)
    for p, (axis, d) in enumerate(offsets):
        copy(p, target(axis, d)).wait_send()


def feed_kernel(mixed_ref, nodes_ref, w_out_ref, gain_ref, w_up_ref, w_down_ref, out_ref):
    mixed_t = mixed_ref[...].reshape(nodes_ref.shape[1], nodes_ref.shape[0])
    residual = nodes_ref[...].astype(jnp.float32) + dot(mixed_t.T, w_out_ref[...])
    normed = normalize(residual, gain_ref[...])
    upward = dot(normed, w_up_ref[...])
    activated = jax.nn.gelu(upward, approximate=True).astype(jnp.bfloat16)
    out_ref[...] = (residual + dot(activated, w_down_ref[...])).astype(jnp.bfloat16)


def shards(
    row_size, col_size,
    nodes, ln1_gain, w_qkv, w_out, ln2_gain, w_up, w_down, adjacency, remote_ids, remote_live
):
    rows, width = nodes.shape
    count = row_size + col_size - 2
    group = 2 if count % 2 == 0 else 1
    vmem = pl.BlockSpec(memory_space=pltpu.VMEM)
    smem = pl.BlockSpec(memory_space=pltpu.SMEM)
    hbm = pl.BlockSpec(memory_space=pl.ANY)
    bf16, f32 = jnp.bfloat16, jnp.float32
    mixed = pl.pallas_call(
        functools.partial(attention_kernel, row_size, col_size),
        out_shape=jax.ShapeDtypeStruct((HEADS, HEAD_DIM, rows), bf16),
        in_specs=[smem, smem, hbm, vmem, hbm, hbm],
        out_specs=vmem,
        scratch_shapes=[
            pltpu.VMEM((rows, width), bf16),
            pltpu.VMEM(w_qkv.shape, bf16),
            pltpu.VMEM(adjacency.shape, adjacency.dtype),
            pltpu.VMEM((count, BLK, width), bf16),
            pltpu.VMEM((count, BLK, width), bf16),
            pltpu.SMEM((count,), f32),
            pltpu.VMEM((width, width), bf16),
            pltpu.VMEM((width, width), bf16),
            pltpu.VMEM((HEADS, 2 * HEAD_DIM, rows), bf16),
            pltpu.VMEM((HEADS // 2, rows, BLK), bf16),
            pltpu.VMEM((HEADS, AUG, rows), bf16),
            pltpu.VMEM((HEADS // 2, group * BLK, BLK), bf16),
            pltpu.VMEM((HEADS, AUG, group * BLK), bf16),
            pltpu.VMEM((BLK, rows), f32),
            pltpu.VMEM((HEADS, 1, rows), f32),
            pltpu.VMEM((HEADS, AUG, rows), f32),
            pltpu.SemaphoreType.DMA((count,)),
            pltpu.SemaphoreType.DMA((count,)),
            pltpu.SemaphoreType.DMA((3,)),
        ],
        compiler_params=pltpu.CompilerParams(
            collective_id=0, has_side_effects=True, vmem_limit_bytes=60 << 20
        ),
        name="attention",
    )(remote_ids, remote_live, nodes, ln1_gain.reshape(1, width), w_qkv, adjacency)
    chunk = 2 * BLK
    hidden = w_up.shape[1]
    whole = lambda *dims: pl.BlockSpec(dims, lambda i: (0,) * len(dims))
    return pl.pallas_call(
        feed_kernel,
        grid=(rows // chunk,),
        out_shape=jax.ShapeDtypeStruct((rows, width), bf16),
        in_specs=[
            pl.BlockSpec((HEADS, HEAD_DIM, chunk), lambda i: (0, 0, i)),
            pl.BlockSpec((chunk, width), lambda i: (i, 0)),
            whole(width, width),
            whole(1, width),
            whole(width, hidden),
            whole(hidden, width),
        ],
        out_specs=pl.BlockSpec((chunk, width), lambda i: (i, 0)),
        compiler_params=pltpu.CompilerParams(vmem_limit_bytes=40 << 20),
        name="feed",
    )(mixed, nodes, w_out, ln2_gain.reshape(1, width), w_up, w_down)


def solution(mesh):
    split = P(("row", "col"), None)
    return jax.shard_map(
        functools.partial(shards, mesh.shape["row"], mesh.shape["col"]),
        mesh=mesh,
        in_specs=(split, P(), P(), P(), P(), P(), P(), split, P(), P()),
        out_specs=split,
        check_vma=False,
    )
```
